32 devices in a mesh: dp: 4 (over x, core), mp: 8 (over z, y).
Axes of the slice: x: 2, y: 2, z: 4, core: 2. Of those that a mesh axis runs over, the one named last changes fastest.
Arguments:
- tokens: bfloat16 [256, 8192], P('dp', 'mp'), may hold values from -80 to 80
- frozen_gate_weight: bfloat16 [8192, 28672], P('mp', 'dp'), may hold values from -0.198873782 to 0.198873782
- frozen_up_weight: bfloat16 [8192, 28672], P('mp', 'dp'), may hold values from -0.198873782 to 0.198873782
- frozen_down_weight: bfloat16 [28672, 8192], P('dp', 'mp'), may hold values from -0.28347335 to 0.28347335
- gate_left_factor: bfloat16 [8192, 16], P('mp'), may hold values from -0.0625 to 0.0625
- gate_right_factor: bfloat16 [16, 28672], P(None, 'dp'), may hold values from -0.75 to 0.75
- up_left_factor: bfloat16 [8192, 16], P('mp'), may hold values from -0.0625 to 0.0625
- up_right_factor: bfloat16 [16, 28672], P(None, 'dp'), may hold values from -0.75 to 0.75
- down_left_factor: bfloat16 [28672, 16], P('dp'), may hold values from -0.03125 to 0.03125
- down_right_factor: bfloat16 [16, 8192], P(None, 'mp'), may hold values from -0.75 to 0.75
- gate_column_magnitude: float32 [28672], P('dp'), may hold values from 0.5 to 2
- up_column_magnitude: float32 [28672], P('dp'), may hold values from 0.5 to 2
- down_column_magnitude: float32 [8192], P('mp'), may hold values from 0.5 to 2
- cotangent: bfloat16 [256, 8192], P('dp', 'mp'), may hold values from -80 to 80
Outputs:
- feedforward_output: bfloat16 [256, 8192], P('dp', 'mp')
- token_input_gradient: bfloat16 [256, 8192], P('dp', 'mp')
- gate_magnitude_gradient: float32 [28672], P('dp')
- up_magnitude_gradient: float32 [28672], P('dp')
- down_magnitude_gradient: float32 [8192], P('mp')
- gate_right_factor_gradient: float32 [16, 28672], P(None, 'dp')
- gate_left_factor_gradient: float32 [8192, 16], P('mp')
- up_right_factor_gradient: float32 [16, 28672], P(None, 'dp')
- up_left_factor_gradient: float32 [8192, 16], P('mp')
- down_right_factor_gradient: float32 [16, 8192], P(None, 'mp')
- down_left_factor_gradient: float32 [28672, 16], P('dp')
The draws below stay inside these ranges and needn't reach their ends.
All inputs are finite; a program needn't handle non-finite values.
Results may differ from the reference program's by a relative error of at most 0.03.
Values may be sent and summed in bfloat16 or wider, within the bound.
No kernel may reach another device: no remote copies, remote signals or barrier semaphores. Data moves between devices by JAX's collectives and lax.ppermute only.
A program may use at most 192 MiB of HBM per device.

```python
import math
import jax
import jax.numpy as jnp
from jax import lax

MODEL_WIDTH = 8192
HIDDEN_UNITS = 28672
ADAPTER_RANK = 16
TOKENS = 256
N_MP = 8


def scaled_rows(key, num_rows, num_cols, base, salt, steep):
    noise_key, scale_key, column_key = jax.random.split(jax.random.fold_in(key, salt), 3)
    noise = jnp.clip(jax.random.normal(noise_key, (num_rows, num_cols), jnp.float32), -4.0, 4.0)
    spread = 0.5756463
    position = jnp.arange(num_rows, dtype=jnp.float32) / max(num_rows - 1, 1)
    if steep > 0:
        rising = jnp.exp(2.0794415 * (position - 0.5))
    elif steep < 0:
        rising = jnp.exp(-2.0794415 * (position - 0.5))
    else:
        rising = jnp.sqrt((1.0 + 2.0 * position) / 2.0)
    jitter = jnp.exp(jax.random.uniform(scale_key, (num_rows,), jnp.float32, -spread, spread))
    column_scale = jnp.exp(jax.random.uniform(column_key, (num_cols,), jnp.float32, -0.7, 0.7))
    return noise * (rising * jitter * base)[:, None] * column_scale[None, :]


def draw_tokens(key, part):
    return scaled_rows(key, TOKENS, MODEL_WIDTH, 1.0, 101, 1).astype(jnp.bfloat16)


def draw_cotangent(key, part):
    return scaled_rows(key, TOKENS, MODEL_WIDTH, 1.0, 202, -1).astype(jnp.bfloat16)


def draw_frozen_gate_weight(key, part):
    return scaled_rows(key, MODEL_WIDTH, HIDDEN_UNITS, MODEL_WIDTH ** (-0.5), 303, 0).astype(jnp.bfloat16)


def draw_frozen_up_weight(key, part):
    return scaled_rows(key, MODEL_WIDTH, HIDDEN_UNITS, MODEL_WIDTH ** (-0.5), 404, 0).astype(jnp.bfloat16)


def draw_frozen_down_weight(key, part):
    return scaled_rows(key, HIDDEN_UNITS, MODEL_WIDTH, HIDDEN_UNITS ** (-0.5), 505, 1).astype(jnp.bfloat16)


def block_levels(stream_key, dims, cuts, smallest, top_value):
    loudness = 1.0
    for axis_at, parts in cuts:
        heights = jax.random.uniform(jax.random.fold_in(jax.random.fold_in(stream_key, 6), axis_at), (parts,), jnp.float32, smallest / len(cuts), top_value / len(cuts))
        loudness = loudness * jnp.repeat(jnp.exp(heights), dims[axis_at] // parts).reshape((-1,) + (1,) * (len(dims) - 1 - axis_at))
    return loudness


def normal_values(rng, shape, deviation, most, pieces=(), kind=jnp.bfloat16):
    gain = block_levels(rng, shape, pieces, -0.22, 0.18) if pieces else 1.0
    drawn = jax.random.normal(rng, shape, jnp.float32) * deviation * gain
    return jnp.minimum(jnp.maximum(drawn, -most), most).astype(kind)


def setup_inputs(seed: int = 0) -> dict:
    splits = jax.random.split(jax.random.key(seed), 15)
    tokens = draw_tokens(jax.random.fold_in(splits[14], 71), 0)
    frozen_gate_weight = draw_frozen_gate_weight(jax.random.fold_in(splits[14], 71), 0)
    frozen_up_weight = draw_frozen_up_weight(jax.random.fold_in(splits[14], 71), 0)
    frozen_down_weight = draw_frozen_down_weight(jax.random.fold_in(splits[14], 71), 0)
    gate_left_factor = normal_values(splits[4], (MODEL_WIDTH, ADAPTER_RANK), MODEL_WIDTH ** -0.5, 0.0625, ((0, 8),))
    gate_right_factor = normal_values(splits[5], (ADAPTER_RANK, HIDDEN_UNITS), (4 * ADAPTER_RANK) ** -0.5, 0.75, ((1, 4),))
    up_left_factor = normal_values(splits[6], (MODEL_WIDTH, ADAPTER_RANK), MODEL_WIDTH ** -0.5, 0.0625, ((0, 8),))
    up_right_factor = normal_values(splits[7], (ADAPTER_RANK, HIDDEN_UNITS), (4 * ADAPTER_RANK) ** -0.5, 0.75, ((1, 4),))
    down_left_factor = normal_values(splits[8], (HIDDEN_UNITS, ADAPTER_RANK), HIDDEN_UNITS ** -0.5, 0.03125, ((0, 4),))
    down_right_factor = normal_values(splits[9], (ADAPTER_RANK, MODEL_WIDTH), (4 * ADAPTER_RANK) ** -0.5, 0.75, ((1, 8),))
    gate_column_magnitude = jnp.clip(jnp.exp(math.log(2.0) - 1.3862944 * jax.random.uniform(splits[10], (HIDDEN_UNITS,), jnp.float32) ** block_levels(splits[10], (HIDDEN_UNITS,), ((0, 4),), -0.2, 0.2)), 0.5, 2.0)
    up_column_magnitude = jnp.clip(jnp.exp(math.log(2.0) - 1.3862944 * jax.random.uniform(splits[11], (HIDDEN_UNITS,), jnp.float32) ** block_levels(splits[11], (HIDDEN_UNITS,), ((0, 4),), -0.2, 0.2)), 0.5, 2.0)
    down_column_magnitude = jnp.clip(jnp.exp(math.log(2.0) - 1.3862944 * jax.random.uniform(splits[12], (MODEL_WIDTH,), jnp.float32) ** block_levels(splits[12], (MODEL_WIDTH,), ((0, 8),), -0.2, 0.2)), 0.5, 2.0)
    cotangent = draw_cotangent(jax.random.fold_in(splits[14], 71), 0)
    return {"tokens": tokens, "frozen_gate_weight": frozen_gate_weight, "frozen_up_weight": frozen_up_weight, "frozen_down_weight": frozen_down_weight, "gate_left_factor": gate_left_factor, "gate_right_factor": gate_right_factor, "up_left_factor": up_left_factor, "up_right_factor": up_right_factor, "down_left_factor": down_left_factor, "down_right_factor": down_right_factor, "gate_column_magnitude": gate_column_magnitude, "up_column_magnitude": up_column_magnitude, "down_column_magnitude": down_column_magnitude, "cotangent": cotangent}


epsilon = 1e-06

def combine_adapter_columns(weight_matrix, left_factor, right_factor):
    combined_weight = weight_matrix.astype(jnp.float32) + jnp.dot(left_factor, right_factor, preferred_element_type=jnp.float32)
    norms = jnp.sqrt(lax.optimization_barrier(jnp.sum(combined_weight * combined_weight, axis=0)) + epsilon)
    return (combined_weight.astype(jnp.bfloat16), norms)

def blocked_product(left_side, right_side, blocks):
    inner = left_side.shape[1] // blocks
    left_blocks = left_side.reshape(left_side.shape[0], blocks, inner).transpose(1, 0, 2)
    right_blocks = right_side.reshape(blocks, inner, right_side.shape[1])

    def blocked_step(running, operands):
        partial_sum = jnp.dot(operands[0], operands[1], preferred_element_type=jnp.float32)
        rounded = lax.optimization_barrier(partial_sum.astype(jnp.bfloat16))
        return (running + rounded.astype(jnp.float32), None)
    start_value = jnp.zeros((left_side.shape[0], right_side.shape[1]), jnp.float32)
    running, _ = lax.scan(blocked_step, start_value, (left_blocks, right_blocks))
    return running

def reference(tokens, frozen_gate_weight, frozen_up_weight, frozen_down_weight, gate_left_factor, gate_right_factor, up_left_factor, up_right_factor, down_left_factor, down_right_factor, gate_column_magnitude, up_column_magnitude, down_column_magnitude, cotangent):
    gate_half_precision, gate_column_norm = combine_adapter_columns(frozen_gate_weight, gate_left_factor, gate_right_factor)
    up_half_precision, up_column_norm = combine_adapter_columns(frozen_up_weight, up_left_factor, up_right_factor)
    down_half_precision, down_column_norm = combine_adapter_columns(frozen_down_weight, down_left_factor, down_right_factor)
    scale_gate = gate_column_magnitude / gate_column_norm
    scale_up = up_column_magnitude / up_column_norm
    scale_down = down_column_magnitude / down_column_norm
    pre_gate = blocked_product(tokens, gate_half_precision, N_MP)
    pre_up = blocked_product(tokens, up_half_precision, N_MP)
    gate_act = pre_gate * scale_gate
    up_act = pre_up * scale_up
    sigmoid_gate = jax.nn.sigmoid(gate_act)
    silu_gate = gate_act * sigmoid_gate
    hidden_state = (silu_gate * up_act).astype(jnp.bfloat16)
    down_preactivation = jnp.dot(hidden_state, down_half_precision, preferred_element_type=jnp.float32)
    feedforward_output = (down_preactivation * scale_down).astype(jnp.bfloat16)
    output_cotangent = cotangent.astype(jnp.float32)
    down_logits = (output_cotangent * scale_down).astype(jnp.bfloat16)
    down_magnitude_gradient = lax.optimization_barrier(jnp.sum(output_cotangent * down_preactivation, axis=0)) / down_column_norm
    grad_hidden = blocked_product(down_logits, down_half_precision.T, N_MP)
    grad_gate = grad_hidden * up_act * sigmoid_gate * (1.0 + gate_act * (1.0 - sigmoid_gate))
    grad_up = grad_hidden * silu_gate
    gate_logits = (grad_gate * scale_gate).astype(jnp.bfloat16)
    up_logits = (grad_up * scale_up).astype(jnp.bfloat16)
    gate_magnitude_gradient = lax.optimization_barrier(jnp.sum(grad_gate * pre_gate, axis=0)) / gate_column_norm
    up_magnitude_gradient = lax.optimization_barrier(jnp.sum(grad_up * pre_up, axis=0)) / up_column_norm
    token_input_gradient = (jnp.dot(gate_logits, gate_half_precision.T, preferred_element_type=jnp.float32) + jnp.dot(up_logits, up_half_precision.T, preferred_element_type=jnp.float32)).astype(jnp.bfloat16)
    gate_projection_output = jnp.dot(tokens, gate_left_factor, preferred_element_type=jnp.float32).astype(jnp.bfloat16)
    up_projection_output = jnp.dot(tokens, up_left_factor, preferred_element_type=jnp.float32).astype(jnp.bfloat16)
    down_projection_output = jnp.dot(hidden_state, down_left_factor, preferred_element_type=jnp.float32).astype(jnp.bfloat16)
    gate_backward_rows = jnp.dot(gate_logits, gate_right_factor.T, preferred_element_type=jnp.float32).astype(jnp.bfloat16)
    up_backward_rows = jnp.dot(up_logits, up_right_factor.T, preferred_element_type=jnp.float32).astype(jnp.bfloat16)
    down_backward_rows = jnp.dot(down_logits, down_right_factor.T, preferred_element_type=jnp.float32).astype(jnp.bfloat16)
    gate_right_factor_gradient = jnp.dot(gate_projection_output.T, gate_logits, preferred_element_type=jnp.float32)
    up_right_factor_gradient = jnp.dot(up_projection_output.T, up_logits, preferred_element_type=jnp.float32)
    down_right_factor_gradient = jnp.dot(down_projection_output.T, down_logits, preferred_element_type=jnp.float32)
    gate_left_factor_gradient = jnp.dot(tokens.T, gate_backward_rows, preferred_element_type=jnp.float32)
    up_left_factor_gradient = jnp.dot(tokens.T, up_backward_rows, preferred_element_type=jnp.float32)
    down_left_factor_gradient = jnp.dot(hidden_state.T, down_backward_rows, preferred_element_type=jnp.float32)
    return (feedforward_output, token_input_gradient, gate_magnitude_gradient, up_magnitude_gradient, down_magnitude_gradient, gate_right_factor_gradient, gate_left_factor_gradient, up_right_factor_gradient, up_left_factor_gradient, down_right_factor_gradient, down_left_factor_gradient)
```

```python
import itertools

import jax
import jax.numpy as jnp
from jax import lax
from jax.experimental import pallas as pl
from jax.experimental.pallas import tpu as pltpu
from jax.sharding import PartitionSpec as P

epsilon = 1e-06
f32 = jnp.float32
bf16 = jnp.bfloat16


SHARES = 14
CHUNKS = ((2, 0, 0), (3, 0, 0), (2, 0, 0), (2, 0, 0), (3, 0, 1), (2, 0, 0))

STATS = 8


def pack(stats):
    high = stats.astype(bf16)
    low = (stats - high.astype(f32)).astype(bf16)
    return jnp.concatenate([high, low, jnp.zeros((STATS - 4, stats.shape[1]), bf16)], axis=0)


def unpack(rows):
    return rows[:2].astype(f32) + rows[2:4].astype(f32)


def dot(a, b, ca, cb):
    return lax.dot_general(a, b, (((ca,), (cb,)), ((), ())), preferred_element_type=f32)


def tile_of(width, most):
    best = width
    for t in range(128, most + 1, 128):
        if width % t == 0:
            best = t
    return best


def call(kernel, grid, in_specs, out_specs, out_shape, flops, nbytes, scratch=()):
    return pl.pallas_call(
        kernel,
        grid=grid,
        in_specs=in_specs,
        out_specs=out_specs,
        out_shape=out_shape,
        scratch_shapes=scratch,
        compiler_params=pltpu.CompilerParams(dimension_semantics=("arbitrary",)),
        cost_estimate=pl.CostEstimate(flops=flops, bytes_accessed=nbytes, transcendentals=0),
    )


def down_norm(w, left, right):
    rows, cols = w.shape
    rank = left.shape[1]
    t = tile_of(rows, 1024)

    def kernel(w_ref, l_ref, r_ref, o_ref):
        m = w_ref[...].astype(f32) + dot(l_ref[...], r_ref[...], 1, 0)
        s = jnp.sum(m * m, axis=0, keepdims=True)

        @pl.when(pl.program_id(0) == 0)
        def _():
            o_ref[...] = s

        @pl.when(pl.program_id(0) > 0)
        def _():
            o_ref[...] += s

    return call(
        kernel,
        (rows // t,),
        [
            pl.BlockSpec((t, cols), lambda i: (i, 0)),
            pl.BlockSpec((t, rank), lambda i: (i, 0)),
            pl.BlockSpec((rank, cols), lambda i: (0, 0)),
        ],
        pl.BlockSpec((1, cols), lambda i: (0, 0)),
        jax.ShapeDtypeStruct((1, cols), f32),
        flops=rows * cols * 500,
        nbytes=rows * cols * 2,
    )(w, left, right)


def partial_chunk(x, z, wg, wu, wd, lg, lu, ld, rg, ru, rd, start, width):
    tokens, depth = x.shape
    rank = lg.shape[1]
    t = tile_of(width, 512)
    off = start // t
    group = tokens // 2

    def kernel(x_ref, z_ref, wg_ref, wu_ref, wd_ref, lg_ref, lu_ref, ld_ref, rg_ref, ru_ref, rd_ref, own, sent, s_ref):
        def put(k, y):
            y = y.astype(bf16)
            own[k * group : (k + 1) * group] = y[:group]
            sent[k * group : (k + 1) * group] = y[group:]

        sums = []
        for k, (w_ref, l_ref, r_ref) in enumerate(((wg_ref, lg_ref, rg_ref), (wu_ref, lu_ref, ru_ref))):
            m = w_ref[...].astype(f32) + dot(l_ref[...], r_ref[...], 1, 0)
            sums.append(jnp.sum(m * m, axis=0, keepdims=True))
            put(k, dot(x_ref[...], m.astype(bf16), 1, 0))
        m = wd_ref[...].astype(f32) + dot(ld_ref[...], rd_ref[...], 1, 0)
        put(2, dot(z_ref[...], m.astype(bf16), 1, 1))
        sums = jnp.concatenate(sums, axis=0)
        s_ref[...] = sums
        sent[3 * group :] = pack(sums)

    whole = lambda shape: pl.BlockSpec(shape, lambda j: (0,) * len(shape))
    wspec = pl.BlockSpec((depth, t), lambda j: (0, off + j))
    rspec = pl.BlockSpec((rank, t), lambda j: (0, off + j))
    down = lambda n: pl.BlockSpec((t, n), lambda j: (off + j, 0))
    columns = lambda n: pl.BlockSpec((n, t), lambda j: (0, j))
    return call(
        kernel,
        (width // t,),
        [whole((tokens, depth)), whole((tokens, depth)), wspec, wspec, down(depth)]
        + [whole((depth, rank)), whole((depth, rank)), down(rank), rspec, rspec, whole((rank, depth))],
        [columns(3 * group), columns(3 * group + STATS), columns(2)],
        [
            jax.ShapeDtypeStruct((3 * group, width), bf16),
            jax.ShapeDtypeStruct((3 * group + STATS, width), bf16),
            jax.ShapeDtypeStruct((2, width), f32),
        ],
        flops=6 * tokens * depth * width,
        nbytes=depth * width * 6,
    )(x, z, wg, wu, wd, lg, lu, ld, rg, ru, rd)


def columnwise(kernel, ins, outs):
    width = ins[0].shape[1]
    t = tile_of(width, 512)
    spec = lambda n: pl.BlockSpec((n, t), lambda j: (0, j))
    nbytes = sum(a.size * a.dtype.itemsize for a in ins)
    return call(
        kernel,
        (width // t,),
        [spec(a.shape[0]) for a in ins],
        [spec(n) for n, _ in outs],
        [jax.ShapeDtypeStruct((n, width), dt) for n, dt in outs],
        flops=nbytes,
        nbytes=2 * nbytes,
    )(*ins)


def add_halves(own, got, stats):
    rows = own.shape[0] // 6

    def kernel(own_ref, got_ref, stats_ref, keep, send, out):
        for k in range(3):
            lo, mid = 2 * k * rows, (2 * k + 1) * rows
            keep[k * rows : (k + 1) * rows] = (
                own_ref[lo:mid].astype(f32) + got_ref[lo:mid].astype(f32)
            ).astype(bf16)
            send[k * rows : (k + 1) * rows] = (
                own_ref[mid : mid + rows].astype(f32) + got_ref[mid : mid + rows].astype(f32)
            ).astype(bf16)
        total = stats_ref[...] + unpack(got_ref[6 * rows :])
        out[...] = total
        send[3 * rows :] = pack(total)

    return columnwise(kernel, (own, got, stats), ((3 * rows, bf16), (3 * rows + STATS, bf16), (2, f32)))


def activate(own, got, stats, magnitudes):
    rb = own.shape[0] // 3

    def kernel(own_ref, got_ref, stats_ref, mag_ref, load, norm_ref, part_ref):
        norm2 = jnp.sqrt(stats_ref[...] + unpack(got_ref[3 * rb :]) + epsilon)
        norm_ref[...] = norm2
        scale = mag_ref[...] / norm2
        sg, su = scale[0:1], scale[1:2]
        total = lambda k: own_ref[k * rb : (k + 1) * rb].astype(f32) + got_ref[k * rb : (k + 1) * rb].astype(f32)
        pre_gate, pre_up, grad_hidden = total(0), total(1), total(2)
        gate_act = pre_gate * sg
        up_act = pre_up * su
        sig = jax.nn.sigmoid(gate_act)
        silu = gate_act * sig
        grad_gate = grad_hidden * up_act * sig * (1.0 + gate_act * (1.0 - sig))
        grad_up = grad_hidden * silu
        load[:rb] = (silu * up_act).astype(bf16)
        load[rb : 2 * rb] = (grad_gate * sg).astype(bf16)
        load[2 * rb : 3 * rb] = (grad_up * su).astype(bf16)
        part = jnp.concatenate(
            [jnp.sum(grad_gate * pre_gate, axis=0, keepdims=True), jnp.sum(grad_up * pre_up, axis=0, keepdims=True)],
            axis=0,
        )
        part_ref[...] = part
        load[3 * rb :] = pack(part)

    return columnwise(kernel, (own, got, stats, magnitudes), ((3 * rb + STATS, bf16), (2, f32), (2, f32)))


def join(load, got, part):
    rows = load.shape[0] - STATS

    def kernel(load_ref, got_ref, part_ref, both, out):
        both[:rows] = load_ref[:rows]
        both[rows : 2 * rows] = got_ref[:rows]
        total = part_ref[...] + unpack(got_ref[rows:])
        out[...] = total
        both[2 * rows :] = pack(total)

    return columnwise(kernel, (load, got, part), ((2 * rows + STATS, bf16), (2, f32)))


def backward_chunk(pieces, part, norm2, places, rb, wg, wu, wd, lg, lu, ld, rg, ru, rd, pg, pu, bd, acc, start, width):
    half = len(places) // 2
    depth = wg.shape[0]
    rank = lg.shape[1]
    tokens = 2 * half * rb
    t = tile_of(width, 512)
    off = start // t
    first = acc is None

    def kernel(*refs):
        ps = refs[:2]
        wg_ref, wu_ref, wd_ref, lg_ref, lu_ref, ld_ref, rg_ref, ru_ref, rd_ref, pg_ref, pu_ref, bd_ref = refs[2:14]
        part_ref, norm_ref = refs[14:16]
        ins = refs[16:-7]
        down_ref, dx_ref, small_ref, gr_ref, ur_ref, dl_ref, mag_ref = refs[-7:]
        mag_ref[...] = (part_ref[...] + unpack(ps[1][3 * half * rb :])) / norm_ref[...]

        def rows(k):
            at = lambda q: ((q % half) * 3 + k) * rb
            return jnp.concatenate([ps[q // half][at(q) : at(q) + rb] for q in places], axis=0)

        h, zg, zu = rows(0), rows(1), rows(2)

        def merged(w_ref, l_ref, r_ref):
            return (w_ref[...].astype(f32) + dot(l_ref[...], r_ref[...], 1, 0)).astype(bf16)

        @pl.when(pl.program_id(0) == 0)
        def _():
            for k, ref in enumerate((down_ref, dx_ref, small_ref)):
                ref[...] = jnp.zeros(ref.shape, f32) if first else ins[k][...]

        down_ref[...] += dot(h, merged(wd_ref, ld_ref, rd_ref), 1, 0)
        dx_ref[...] += dot(zg, merged(wg_ref, lg_ref, rg_ref), 1, 1) + dot(zu, merged(wu_ref, lu_ref, ru_ref), 1, 1)
        small_ref[:rank] += dot(ld_ref[...], h, 0, 1)
        small_ref[rank : 2 * rank] += dot(rg_ref[...], zg, 1, 1)
        small_ref[2 * rank :] += dot(ru_ref[...], zu, 1, 1)
        gr_ref[...] = dot(pg_ref[...], zg, 0, 0)
        ur_ref[...] = dot(pu_ref[...], zu, 0, 0)
        dl_ref[...] = dot(h, bd_ref[...], 0, 0)

    whole = lambda shape: pl.BlockSpec(shape, lambda j: (0,) * len(shape))
    wspec = pl.BlockSpec((depth, t), lambda j: (0, off + j))
    rspec = pl.BlockSpec((rank, t), lambda j: (0, off + j))
    rows_spec = lambda n: pl.BlockSpec((t, n), lambda j: (off + j, 0))
    sums = [(tokens, wd.shape[1]), (tokens, depth), (3 * rank, tokens)]
    ins = [] if first else list(acc)
    return call(
        kernel,
        (width // t,),
        [pl.BlockSpec((p.shape[0], t), lambda j: (0, j)) for p in pieces]
        + [wspec, wspec, rows_spec(wd.shape[1])]
        + [whole((depth, rank)), whole((depth, rank)), rows_spec(rank)]
        + [rspec, rspec, whole((rank, wd.shape[1]))]
        + [whole((tokens, rank))] * 3
        + [pl.BlockSpec((2, t), lambda j: (0, j))] * 2
        + [whole(a.shape) for a in ins],
        [whole(s) for s in sums]
        + [pl.BlockSpec((rank, t), lambda j: (0, j))] * 2
        + [pl.BlockSpec((t, rank), lambda j: (j, 0)), pl.BlockSpec((2, t), lambda j: (0, j))],
        [jax.ShapeDtypeStruct(s, f32) for s in sums + [(rank, width), (rank, width), (width, rank), (2, width)]],
        flops=6 * tokens * depth * width,
        nbytes=depth * width * 6,
    )(*pieces, wg, wu, wd, lg, lu, ld, rg, ru, rd, pg, pu, bd, part, norm2, *ins)


def masks_of(bits):
    return [sum(b for b, on in zip(bits, flags) if on) for flags in itertools.product((0, 1), repeat=len(bits))]


def place_of(mask, bits):
    return sum(((mask // b) % 2) << (len(bits) - 1 - k) for k, b in enumerate(bits))


def powers(n):
    return [1 << k for k in range(n.bit_length() - 1)]


def per_device(
    tokens,
    wg,
    wu,
    wd,
    lg,
    rg,
    lu,
    ru,
    ld,
    rd,
    gate_column_magnitude,
    up_column_magnitude,
    down_column_magnitude,
    cotangent,
):
    n_mp = lax.axis_size("mp")
    n_dp = lax.axis_size("dp")
    m = lax.axis_index("mp")
    i_dp = lax.axis_index("dp")
    bits = powers(n_mp)
    dbits = powers(n_dp)
    swapped = [bits[1], bits[0]] + bits[2:]
    tl = tokens.shape[0]
    total = tl * n_dp
    rb = total // n_mp
    hl = wg.shape[1]
    rank = lg.shape[1]
    unit = hl // SHARES

    def swap(a, axis, bit):
        return lax.ppermute(a, axis, [(k, k ^ bit) for k in range(lax.axis_size(axis))])

    def total_over(a, axis, axis_bits):
        for b in axis_bits:
            a = (a.astype(f32) + swap(a, axis, b).astype(f32)).astype(a.dtype)
        return a

    def blocks(a, places, size, axis=0):
        return jnp.concatenate([lax.dynamic_slice_in_dim(a, p, size, axis) for p in places], axis=axis)

    def in_order(a, order):
        return blocks(a, [(m ^ k) * rb for k in masks_of(order)], rb)

    both = jnp.stack([tokens, cotangent])[None]
    for b in reversed(dbits):
        both = jnp.concatenate([both, swap(both, "dp", b)], axis=0)

    def everyone(k):
        return blocks(both[:, k].reshape(total, -1), [place_of(i_dp ^ d, dbits) * tl for d in range(n_dp)], tl)

    x, cot = everyone(0), everyone(1)

    down_sq = down_norm(wd, ld, rd)
    norm_down = jnp.sqrt(total_over(down_sq, "dp", dbits) + epsilon)
    scale_down = down_column_magnitude[None, :] / norm_down
    z_down = (cot.astype(f32) * scale_down).astype(bf16)

    small = jnp.concatenate([dot(lg, x, 0, 1), dot(lu, x, 0, 1), dot(rd, z_down, 1, 1)], axis=0).astype(bf16)
    small = in_order(total_over(small, "mp", bits[::-1]).T, bits)
    pg, pu, bd = small[:, :rank], small[:, rank : 2 * rank], small[:, 2 * rank :]

    magnitudes = jnp.stack([gate_column_magnitude, up_column_magnitude])
    starts, state = [], []
    start = 0
    for share, swapping, _ in CHUNKS:
        width = share * unit
        order = swapped if swapping else bits
        own, sent, sq = partial_chunk(
            in_order(x, order), in_order(z_down, order), wg, wu, wd, lg, lu, ld, rg, ru, rd, start, width
        )
        for k, b in enumerate(order):
            got = swap(sent, "mp", b)
            if k + 1 < len(order):
                own, sent, sq = add_halves(own, got, sq)
        cols = slice(start, start + width)
        state.append(activate(own, got, sq, magnitudes[:, cols]))
        starts.append(start)
        start += width

    acc = None
    mags, gr, ur, dl = [], [], [], []
    for c, (share, _, swapping) in enumerate(CHUNKS):
        width = share * unit
        order = swapped if swapping else bits
        load, norm2, part = state[c]
        for k, b in enumerate(reversed(order)):
            got = swap(load, "mp", b)
            if k + 1 < len(order):
                load, part = join(load, got, part)
        places = [place_of(k, order) for k in masks_of(bits)]
        *acc, g, u, dleft, mag = backward_chunk(
            (load, got), part, norm2, places, rb, wg, wu, wd, lg, lu, ld, rg, ru, rd, pg, pu, bd, acc, starts[c], width
        )
        mags.append(mag)
        gr.append(g)
        ur.append(u)
        dl.append(dleft)

    mag = jnp.concatenate(mags, axis=1)
    down, dx, back = acc

    mag_down = jnp.sum(in_order(cot, bits).astype(f32) * down, axis=0)
    cols = mag_down.shape[0]
    spare = -(back.size // cols + 1) % 16
    tail = jnp.concatenate(
        [back.astype(bf16).reshape(-1, cols), mag_down.astype(bf16)[None], jnp.zeros((spare, cols), bf16)], axis=0
    )
    owners = [[(i_dp ^ k) * tl // rb + r for r in range(tl // rb)] for k in masks_of(dbits)]
    out = jnp.concatenate(
        [blocks(a, [place_of(m ^ o, bits) * rb for o in group], rb).astype(bf16) for group in owners for a in (down, dx)],
        axis=0,
    )
    for k, b in enumerate(dbits):
        rows = out.shape[0] // 2
        got = swap(jnp.concatenate([out[rows:], tail], axis=0), "dp", b).astype(f32)
        out = out[:rows].astype(f32) + got[:rows]
        tail = tail.astype(f32) + got[rows:]
        if k + 1 < len(dbits):
            out, tail = out.astype(bf16), tail.astype(bf16)
    used = back.size // cols
    mag_down = tail[used]
    back = tail[:used].astype(bf16).reshape(back.shape)

    x_rel = in_order(x, bits)
    z_rel = in_order(z_down, bits)
    return (
        (out[:tl] * scale_down).astype(bf16),
        out[tl:].astype(bf16),
        mag[0],
        mag[1],
        mag_down / norm_down[0],
        jnp.concatenate(gr, axis=1),
        dot(x_rel, back[rank : 2 * rank], 0, 1),
        jnp.concatenate(ur, axis=1),
        dot(x_rel, back[2 * rank :], 0, 1),
        dot(back[:rank], z_rel, 1, 0),
        jnp.concatenate(dl, axis=0),
    )


def solution(mesh):
    placed = (
        P("dp", "mp"),
        P("mp", "dp"),
        P("mp", "dp"),
        P("dp", "mp"),
        P("mp", None),
        P(None, "dp"),
        P("mp", None),
        P(None, "dp"),
        P("dp", None),
        P(None, "mp"),
        P("dp"),
        P("dp"),
        P("mp"),
        P("dp", "mp"),
    )

    return jax.shard_map(
        per_device,
        mesh=mesh,
        in_specs=placed,
        out_specs=(
            P("dp", "mp"),
            P("dp", "mp"),
            P("dp"),
            P("dp"),
            P("mp"),
            P(None, "dp"),
            P("mp", None),
            P(None, "dp"),
            P("mp", None),
            P(None, "mp"),
            P("dp", None),
        ),
        check_vma=False,
    )
```

```python
import itertools

import jax
import jax.numpy as jnp
from jax import lax
from jax.experimental import pallas as pl
from jax.experimental.pallas import tpu as pltpu
from jax.sharding import PartitionSpec as P

epsilon = 1e-06
f32 = jnp.float32
bf16 = jnp.bfloat16


SHARES = 14
TILE = 256
CHUNKS = ((2, 0, 0), (3, 0, 0), (2, 0, 0), (2, 0, 0), (3, 0, 1), (2, 0, 0))

STATS = 8


def pack(stats):
    high = stats.astype(bf16)
    low = (stats - high.astype(f32)).astype(bf16)
    return jnp.concatenate([high, low, jnp.zeros((STATS - 4, stats.shape[1]), bf16)], axis=0)


def unpack(rows):
    return rows[:2].astype(f32) + rows[2:4].astype(f32)


def dot(a, b, ca, cb):
    return lax.dot_general(a, b, (((ca,), (cb,)), ((), ())), preferred_element_type=f32)


def tile_of(width, most):
    best = width
    for t in range(128, most + 1, 128):
        if width % t == 0:
            best = t
    return best


def call(kernel, grid, in_specs, out_specs, out_shape, flops, nbytes, aliases=None):
    return pl.pallas_call(
        kernel,
        grid=grid,
        in_specs=in_specs,
        out_specs=out_specs,
        out_shape=out_shape,
        input_output_aliases=aliases or {},
        compiler_params=pltpu.CompilerParams(dimension_semantics=("arbitrary",)),
        cost_estimate=pl.CostEstimate(flops=flops, bytes_accessed=nbytes, transcendentals=0),
    )


def down_norm(w, left, right):
    rows, cols = w.shape
    rank = left.shape[0]
    t = tile_of(rows, 1024)

    def kernel(w_ref, l_ref, r_ref, o_ref):
        m = w_ref[...].astype(f32) + dot(l_ref[...], r_ref[...], 0, 0)
        s = jnp.sum(m * m, axis=0, keepdims=True)

        @pl.when(pl.program_id(0) == 0)
        def _():
            o_ref[...] = s

        @pl.when(pl.program_id(0) > 0)
        def _():
            o_ref[...] += s

    return call(
        kernel,
        (rows // t,),
        [
            pl.BlockSpec((t, cols), lambda i: (i, 0)),
            pl.BlockSpec((rank, t), lambda i: (0, i)),
            pl.BlockSpec((rank, cols), lambda i: (0, 0)),
        ],
        pl.BlockSpec((1, cols), lambda i: (0, 0)),
        jax.ShapeDtypeStruct((1, cols), f32),
        flops=rows * cols * 500,
        nbytes=rows * cols * 2,
    )(w, left, right)


def partial_chunk(x, z, wg, wu, wd, lg, lu, ld, rg, ru, rd, start, width):
    tokens, depth = x.shape
    rank = lg.shape[0]
    t = tile_of(width, 2 * TILE)
    off = start // t
    group = tokens // 2

    def kernel(x_ref, z_ref, wg_ref, wu_ref, wd_ref, lg_ref, lu_ref, ld_ref, rg_ref, ru_ref, rd_ref, own, sent, s_ref):
        def put(k, y):
            y = y.astype(bf16)
            own[k * group : (k + 1) * group] = y[:group]
            sent[k * group : (k + 1) * group] = y[group:]

        sums = []
        for k, (w_ref, l_ref, r_ref) in enumerate(((wg_ref, lg_ref, rg_ref), (wu_ref, lu_ref, ru_ref))):
            m = w_ref[...].astype(f32) + dot(l_ref[...], r_ref[...], 0, 0)
            sums.append(jnp.sum(m * m, axis=0, keepdims=True))
            put(k, dot(x_ref[...], m.astype(bf16), 1, 0))
        m = wd_ref[...].astype(f32) + dot(ld_ref[...], rd_ref[...], 0, 0)
        put(2, dot(z_ref[...], m.astype(bf16), 1, 1))
        sums = jnp.concatenate(sums, axis=0)
        s_ref[...] = sums
        sent[3 * group :] = pack(sums)

    whole = lambda shape: pl.BlockSpec(shape, lambda j: (0,) * len(shape))
    wspec = pl.BlockSpec((depth, t), lambda j: (0, off + j))
    rspec = pl.BlockSpec((rank, t), lambda j: (0, off + j))
    columns = lambda n: pl.BlockSpec((n, t), lambda j: (0, j))
    return call(
        kernel,
        (width // t,),
        [whole((tokens, depth)), whole((tokens, depth)), wspec, wspec, pl.BlockSpec((t, depth), lambda j: (off + j, 0))]
        + [whole((rank, depth)), whole((rank, depth)), rspec, rspec, rspec, whole((rank, depth))],
        [columns(3 * group), columns(3 * group + STATS), columns(2)],
        [
            jax.ShapeDtypeStruct((3 * group, width), bf16),
            jax.ShapeDtypeStruct((3 * group + STATS, width), bf16),
            jax.ShapeDtypeStruct((2, width), f32),
        ],
        flops=6 * tokens * depth * width,
        nbytes=depth * width * 6,
    )(x, z, wg, wu, wd, lg, lu, ld, rg, ru, rd)


def columnwise(kernel, ins, outs):
    width = ins[0].shape[1]
    t = tile_of(width, 512)
    spec = lambda n: pl.BlockSpec((n, t), lambda j: (0, j))
    nbytes = sum(a.size * a.dtype.itemsize for a in ins)
    return call(
        kernel,
        (width // t,),
        [spec(a.shape[0]) for a in ins],
        [spec(n) for n, _ in outs],
        [jax.ShapeDtypeStruct((n, width), dt) for n, dt in outs],
        flops=nbytes,
        nbytes=2 * nbytes,
    )(*ins)


def add_halves(own, got, stats):
    rows = own.shape[0] // 6

    def kernel(own_ref, got_ref, stats_ref, keep, send, out):
        for k in range(3):
            lo, mid = 2 * k * rows, (2 * k + 1) * rows
            keep[k * rows : (k + 1) * rows] = (
                own_ref[lo:mid].astype(f32) + got_ref[lo:mid].astype(f32)
            ).astype(bf16)
            send[k * rows : (k + 1) * rows] = (
                own_ref[mid : mid + rows].astype(f32) + got_ref[mid : mid + rows].astype(f32)
            ).astype(bf16)
        total = stats_ref[...] + unpack(got_ref[6 * rows :])
        out[...] = total
        send[3 * rows :] = pack(total)

    return columnwise(kernel, (own, got, stats), ((3 * rows, bf16), (3 * rows + STATS, bf16), (2, f32)))


def activate(own, got, stats, magnitudes):
    rb = own.shape[0] // 3

    def kernel(own_ref, got_ref, stats_ref, mag_ref, load, norm_ref, part_ref):
        norm2 = jnp.sqrt(stats_ref[...] + unpack(got_ref[3 * rb :]) + epsilon)
        norm_ref[...] = norm2
        scale = mag_ref[...] / norm2
        sg, su = scale[0:1], scale[1:2]
        total = lambda k: own_ref[k * rb : (k + 1) * rb].astype(f32) + got_ref[k * rb : (k + 1) * rb].astype(f32)
        pre_gate, pre_up, grad_hidden = total(0), total(1), total(2)
        gate_act = pre_gate * sg
        up_act = pre_up * su
        sig = jax.nn.sigmoid(gate_act)
        silu = gate_act * sig
        grad_gate = grad_hidden * up_act * sig * (1.0 + gate_act * (1.0 - sig))
        grad_up = grad_hidden * silu
        load[:rb] = (silu * up_act).astype(bf16)
        load[rb : 2 * rb] = (grad_gate * sg).astype(bf16)
        load[2 * rb : 3 * rb] = (grad_up * su).astype(bf16)
        part = jnp.concatenate(
            [jnp.sum(grad_gate * pre_gate, axis=0, keepdims=True), jnp.sum(grad_up * pre_up, axis=0, keepdims=True)],
            axis=0,
        )
        part_ref[...] = part
        load[3 * rb :] = pack(part)

    return columnwise(kernel, (own, got, stats, magnitudes), ((3 * rb + STATS, bf16), (2, f32), (2, f32)))


def join(load, got, part):
    rows = load.shape[0] - STATS

    def kernel(load_ref, got_ref, part_ref, both, out):
        both[:rows] = load_ref[:rows]
        both[rows : 2 * rows] = got_ref[:rows]
        total = part_ref[...] + unpack(got_ref[rows:])
        out[...] = total
        both[2 * rows :] = pack(total)

    return columnwise(kernel, (load, got, part), ((2 * rows + STATS, bf16), (2, f32)))


def backward_chunk(pieces, part, norm2, places, rb, wg, wu, wd, lg, lu, ld, rg, ru, rd, small, acc, start, width):
    half = len(places) // 2
    depth = wg.shape[0]
    rank = lg.shape[0]
    tokens = 2 * half * rb
    t = tile_of(width, TILE)
    off = start // t
    first = acc is None

    def kernel(*refs):
        ps = refs[:2]
        wg_ref, wu_ref, wd_ref, lg_ref, lu_ref, ld_ref, rg_ref, ru_ref, rd_ref, small_ref = refs[2:12]
        part_ref, norm_ref = refs[12:14]
        ins = refs[14:-4]
        down_ref, dx_ref, back_ref, cols_ref = refs[-4:]
        cols_ref[3 * rank : 3 * rank + 2] = (part_ref[...] + unpack(ps[1][3 * half * rb :])) / norm_ref[...]

        def rows(k):
            at = lambda q: ((q % half) * 3 + k) * rb
            return jnp.concatenate([ps[q // half][at(q) : at(q) + rb] for q in places], axis=0)

        h, zg, zu = rows(0), rows(1), rows(2)

        def merged(w_ref, l_ref, r_ref):
            return (w_ref[...].astype(f32) + dot(l_ref[...], r_ref[...], 0, 0)).astype(bf16)

        @pl.when(pl.program_id(0) == 0)
        def _():
            for k, ref in enumerate((down_ref, dx_ref, back_ref)):
                ref[...] = jnp.zeros(ref.shape, f32) if first else ins[k][...]

        down_ref[...] += dot(h, merged(wd_ref, ld_ref, rd_ref), 1, 0)
        dx_ref[...] += dot(zg, merged(wg_ref, lg_ref, rg_ref), 1, 1) + dot(zu, merged(wu_ref, lu_ref, ru_ref), 1, 1)
        back_ref[:rank] += dot(ld_ref[...], h, 1, 1)
        back_ref[rank : 2 * rank] += dot(rg_ref[...], zg, 1, 1)
        back_ref[2 * rank :] += dot(ru_ref[...], zu, 1, 1)
        for k, v in enumerate((zg, zu, h)):
            cols_ref[k * rank : (k + 1) * rank] = dot(small_ref[k * rank : (k + 1) * rank], v, 1, 0)

    whole = lambda shape: pl.BlockSpec(shape, lambda j: (0,) * len(shape))
    wspec = pl.BlockSpec((depth, t), lambda j: (0, off + j))
    rspec = pl.BlockSpec((rank, t), lambda j: (0, off + j))
    sums = [(tokens, wd.shape[1]), (tokens, depth), (3 * rank, tokens)]
    ins = [] if first else list(acc)
    rows = 3 * rank + 8
    return call(
        kernel,
        (width // t,),
        [pl.BlockSpec((p.shape[0], t), lambda j: (0, j)) for p in pieces]
        + [wspec, wspec, pl.BlockSpec((t, wd.shape[1]), lambda j: (off + j, 0))]
        + [whole((rank, depth)), whole((rank, depth)), rspec]
        + [rspec, rspec, whole((rank, wd.shape[1]))]
        + [whole(small.shape)]
        + [pl.BlockSpec((2, t), lambda j: (0, j))] * 2
        + [whole(a.shape) for a in ins[:3]]
        + [pl.BlockSpec(memory_space=pl.ANY) for a in ins[3:]],
        [whole(s) for s in sums]
        + [pl.BlockSpec((rows, t), lambda j: (0, off + j))],
        [jax.ShapeDtypeStruct(s, f32) for s in sums + [(rows, wg.shape[1])]],
        flops=6 * tokens * depth * width,
        nbytes=depth * width * 6,
        aliases={} if first else {17: 3},
    )(*pieces, wg, wu, wd, lg, lu, ld, rg, ru, rd, small, part, norm2, *ins)


def masks_of(bits):
    return [sum(b for b, on in zip(bits, flags) if on) for flags in itertools.product((0, 1), repeat=len(bits))]


def place_of(mask, bits):
    return sum(((mask // b) % 2) << (len(bits) - 1 - k) for k, b in enumerate(bits))


def powers(n):
    return [1 << k for k in range(n.bit_length() - 1)]


def per_device(
    tokens,
    wg,
    wu,
    wd,
    lg,
    rg,
    lu,
    ru,
    ld,
    rd,
    gate_column_magnitude,
    up_column_magnitude,
    down_column_magnitude,
    cotangent,
):
    n_mp = lax.axis_size("mp")
    n_dp = lax.axis_size("dp")
    m = lax.axis_index("mp")
    i_dp = lax.axis_index("dp")
    bits = powers(n_mp)
    dbits = powers(n_dp)
    swapped = [bits[1], bits[0]] + bits[2:]
    tl = tokens.shape[0]
    total = tl * n_dp
    rb = total // n_mp
    hl = wg.shape[1]
    lg, lu, ld = lg.T, lu.T, ld.T
    rank = lg.shape[0]
    unit = hl // SHARES

    def swap(a, axis, bit):
        return lax.ppermute(a, axis, [(k, k ^ bit) for k in range(lax.axis_size(axis))])

    def total_over(a, axis, axis_bits):
        for b in axis_bits:
            a = (a.astype(f32) + swap(a, axis, b).astype(f32)).astype(a.dtype)
        return a

    def blocks(a, places, size, axis=0):
        return jnp.concatenate([lax.dynamic_slice_in_dim(a, p, size, axis) for p in places], axis=axis)

    def in_order(a, order):
        return blocks(a, [(m ^ k) * rb for k in masks_of(order)], rb)

    def one_hot(places, size):
        rows = jnp.concatenate([p + jnp.arange(size) for p in places])
        return (rows[:, None] == jnp.arange(total)[None, :]).astype(bf16)

    both = jnp.stack([tokens, cotangent])[None]
    for b in reversed(dbits):
        both = jnp.concatenate([both, swap(both, "dp", b)], axis=0)

    def everyone(k):
        return blocks(both[:, k].reshape(total, -1), [place_of(i_dp ^ d, dbits) * tl for d in range(n_dp)], tl)

    x, cot = everyone(0), everyone(1)

    down_sq = down_norm(wd, ld, rd)
    norm_down = jnp.sqrt(total_over(down_sq, "dp", dbits) + epsilon)
    scale_down = down_column_magnitude[None, :] / norm_down
    z_down = (cot.astype(f32) * scale_down).astype(bf16)

    small = jnp.concatenate([dot(lg, x, 1, 1), dot(lu, x, 1, 1), dot(rd, z_down, 1, 1)], axis=0).astype(bf16)
    small = total_over(small, "mp", bits[::-1])
    small = dot(small, one_hot([(m ^ k) * rb for k in masks_of(bits)], rb), 1, 1).astype(bf16)

    magnitudes = jnp.stack([gate_column_magnitude, up_column_magnitude])
    starts, state = [], []
    start = 0
    for share, swapping, _ in CHUNKS:
        width = share * unit
        order = swapped if swapping else bits
        own, sent, sq = partial_chunk(
            in_order(x, order), in_order(z_down, order), wg, wu, wd, lg, lu, ld, rg, ru, rd, start, width
        )
        for k, b in enumerate(order):
            got = swap(sent, "mp", b)
            if k + 1 < len(order):
                own, sent, sq = add_halves(own, got, sq)
        cols = slice(start, start + width)
        state.append(activate(own, got, sq, magnitudes[:, cols]))
        starts.append(start)
        start += width

    acc = None
    for c, (share, _, swapping) in enumerate(CHUNKS):
        width = share * unit
        order = swapped if swapping else bits
        load, norm2, part = state[c]
        for k, b in enumerate(reversed(order)):
            got = swap(load, "mp", b)
            if k + 1 < len(order):
                load, part = join(load, got, part)
        places = [place_of(k, order) for k in masks_of(bits)]
        acc = backward_chunk(
            (load, got), part, norm2, places, rb, wg, wu, wd, lg, lu, ld, rg, ru, rd, small, acc, starts[c], width
        )

    down, dx, back, per_column = acc

    mag_down = jnp.sum(in_order(cot, bits).astype(f32) * down, axis=0)
    cols = mag_down.shape[0]
    used = back.size // cols
    tail = jnp.concatenate([back.astype(bf16).reshape(-1, cols), mag_down.astype(bf16)[None]], axis=0)
    tail = jnp.pad(tail, ((0, -tail.shape[0] % 16), (0, cols)))
    owners = [(i_dp ^ k) * tl // rb + r for k in masks_of(dbits) for r in range(tl // rb)]
    select = one_hot([place_of(m ^ o, bits) * rb for o in owners], rb)
    out = dot(select, jnp.concatenate([down.astype(bf16), dx.astype(bf16)], axis=1), 1, 0).astype(bf16)
    for k, b in enumerate(dbits):
        rows = out.shape[0] // 2
        got = swap(jnp.concatenate([out[rows:], tail], axis=0), "dp", b).astype(f32)
        out = out[:rows].astype(f32) + got[:rows]
        tail = tail.astype(f32) + got[rows:]
        if k + 1 < len(dbits):
            out, tail = out.astype(bf16), tail.astype(bf16)
    mag_down = tail[used, :cols]
    back = tail[:used, :cols].astype(bf16).reshape(back.shape)

    x_rel = in_order(x, bits)
    z_rel = in_order(z_down, bits)
    return (
        (out[:, :cols] * scale_down).astype(bf16),
        out[:, cols:].astype(bf16),
        per_column[3 * rank],
        per_column[3 * rank + 1],
        mag_down / norm_down[0],
        per_column[:rank],
        dot(back[rank : 2 * rank], x_rel, 1, 0).T,
        per_column[rank : 2 * rank],
        dot(back[2 * rank :], x_rel, 1, 0).T,
        dot(back[:rank], z_rel, 1, 0),
        per_column[2 * rank : 3 * rank].T,
    )


def solution(mesh):
    placed = (
        P("dp", "mp"),
        P("mp", "dp"),
        P("mp", "dp"),
        P("dp", "mp"),
        P("mp", None),
        P(None, "dp"),
        P("mp", None),
        P(None, "dp"),
        P("dp", None),
        P(None, "mp"),
        P("dp"),
        P("dp"),
        P("mp"),
        P("dp", "mp"),
    )

    return jax.shard_map(
        per_device,
        mesh=mesh,
        in_specs=placed,
        out_specs=(
            P("dp", "mp"),
            P("dp", "mp"),
            P("dp"),
            P("dp"),
            P("mp"),
            P(None, "dp"),
            P("mp", None),
            P(None, "dp"),
            P("mp", None),
            P(None, "mp"),
            P("dp", None),
        ),
        check_vma=False,
    )
```
